32 devices in a mesh: section: 8 (over z, core), expert: 4 (over y, x).
Axes of the slice: x: 2, y: 2, z: 4, core: 2. Of those that a mesh axis runs over, the one named last changes fastest.
Arguments:
- state: bfloat16 [8, 512, 2048], P('section', 'expert'), may hold values from -6 to 6
- norm_gain: float32 [8, 2048], P('section'), may hold values from 0.25 to 1.75
- expert_in: bfloat16 [8, 4, 2048, 1536], P('section', 'expert'), may hold values from -0.125 to 0.125
- expert_out: bfloat16 [8, 4, 768, 2048], P('section', 'expert'), may hold values from -0.21875 to 0.21875
- route_ids: int32 [3, 8, 512, 6], P(None, 'section', 'expert'), may hold values from 0 to 63, all different within a row
- route_weights: float32 [3, 8, 512, 6], P(None, 'section', 'expert'), may hold values from 0.3 to 3
Outputs:
- state_out: bfloat16 [8, 512, 2048], P('section', 'expert')
The draws below stay inside these ranges and needn't reach their ends.
Inputs may be any that keep to these rules, and one draw needn't show every extreme that they name: `route_ids`: each token names 6 different experts.
All inputs are finite; a program needn't handle non-finite values.
Results may differ from the reference program's by a relative error of at most 0.02.
Values may be sent and summed in bfloat16 or wider, within the bound.
A program may use at most 64 MiB of HBM per device.

```python
import math
from functools import partial
import jax
import jax.numpy as jnp
from jax import lax

D = 2048
ROUTED = 64
TOP = 6
FF = 768
TICKS = 3
TOK_DEV = 128
CAP = 32
EXPERTS = 4
TOKENS = 512
N_SECTION = 8
N_EXPERT = 4


def steps_of(stream_key, extent, pieces, least, high):
    gain, own = 1.0, jax.random.fold_in(stream_key, 6)
    for position, parts in pieces:
        draws = jnp.exp(jax.random.uniform(jax.random.fold_in(own, position), (parts,), jnp.float32, least / len(pieces), high / len(pieces)))
        gain = gain * jnp.repeat(draws, extent[position] // parts).reshape([-1 if axis == position else 1 for axis in range(len(extent))])
    return gain


def choose_distinct(rng, rows, count, top, lift):
    ranking = jax.random.permutation(jax.random.fold_in(rng, 1), count)
    boost = ranking
    for power in range(3):
        boost = boost * boost // count
    boost = boost * lift // count
    lots = jax.random.randint(jax.random.fold_in(rng, 2), (rows, count), 0, 4096) + boost
    fixed_rows = jax.random.permutation(jax.random.fold_in(rng, 3), rows)[jnp.arange(count) % rows]
    lots = jnp.where(jnp.arange(rows)[:, None] == fixed_rows[None, :], 1 << 14, lots)
    priority = lots * count + jnp.arange(count)
    return lax.top_k(priority.astype(jnp.int32), top)[1].astype(jnp.int32)


def noise(stream_key, extent, deviation, most, pieces=(), kind=jnp.bfloat16):
    gain = steps_of(stream_key, extent, pieces, -0.22, 0.18) if pieces else 1.0
    result = jax.random.normal(stream_key, extent, jnp.float32) * deviation * gain
    return jnp.minimum(jnp.maximum(result, -most), most).astype(kind)


def setup_inputs(seed: int = 0) -> dict:
    splits = jax.random.split(jax.random.key(seed), 7)
    state = noise(splits[0], (N_SECTION, TOKENS, D), 1.0, 6.0, ((0, 8), (1, 4)))
    norm_gain = jnp.clip(1.0 + 0.15 * jax.random.normal(splits[1], (N_SECTION, D), jnp.float32), 0.25, 1.75)
    expert_in = noise(splits[2], (N_SECTION, EXPERTS, D, 2 * FF), D ** -0.5, 0.125, ((0, 8), (1, 4)))
    expert_out = noise(splits[3], (N_SECTION, EXPERTS, FF, D), FF ** -0.5, 0.21875, ((0, 8), (1, 4)))
    route_ids = choose_distinct(splits[4], TICKS * N_SECTION * TOKENS, ROUTED, TOP, 1536).reshape((TICKS, N_SECTION, TOKENS, TOP))
    route_weights = jnp.clip(jnp.exp(math.log(3.0) - 2.3025851 * jax.random.uniform(splits[5], (TICKS, N_SECTION, TOKENS, TOP), jnp.float32) ** steps_of(splits[5], (TICKS, N_SECTION, TOKENS, TOP), ((1, 8), (2, 4)), -0.2, 0.2)), 0.3, 3.0)
    return dict(state=state, norm_gain=norm_gain, expert_in=expert_in, expert_out=expert_out, route_ids=route_ids, route_weights=route_weights)


epsilon = 1e-06

def normalize(hidden, gain_row):
    widened = hidden.astype(jnp.float32)
    rescale = lax.rsqrt(lax.optimization_barrier(jnp.mean(widened * widened, axis=-1, keepdims=True)) + epsilon)
    return (widened * rescale * gain_row).astype(jnp.bfloat16)

def slot_tables(chosen, experts, capacity):
    window = jnp.arange(experts, dtype=jnp.int32)
    choice_hits = (chosen[:, :, None] == window[None, None, :]).astype(jnp.int32)
    picked = lax.optimization_barrier(jnp.sum(choice_hits, axis=1))
    rank_table = jnp.cumsum(picked, axis=0) - picked
    kept_table = picked * (rank_table < capacity).astype(jnp.int32)
    slot_index = jnp.arange(capacity, dtype=jnp.int32)
    slot_match = kept_table[:, :, None] * (rank_table[:, :, None] == slot_index[None, None, :]).astype(jnp.int32)
    positions = jnp.arange(chosen.shape[0], dtype=jnp.int32)
    token_at = lax.optimization_barrier(jnp.sum(slot_match * positions[:, None, None], axis=0))
    filled = lax.optimization_barrier(jnp.sum(slot_match, axis=0))
    kept_hits = choice_hits * kept_table[:, None, :]
    kept_choice = lax.optimization_barrier(jnp.sum(kept_hits, axis=2))
    flat_slot = lax.optimization_barrier(jnp.sum(kept_hits * (window[None, None, :] * capacity + rank_table[:, None, :]), axis=2))
    return (token_at, filled, flat_slot, kept_choice)

def expert_forward(token_rows, inner_weight, outer_weight):
    projected = jnp.dot(token_rows, inner_weight, preferred_element_type=jnp.float32)
    hidden_units = outer_weight.shape[0]
    activated = (jax.nn.silu(projected[:, :hidden_units]) * projected[:, hidden_units:]).astype(jnp.bfloat16)
    return jnp.dot(activated, outer_weight, preferred_element_type=jnp.float32).astype(jnp.bfloat16)

def serve_expert(operands):
    arrived, inner_one, outer_one = operands
    token_rows = arrived.reshape(-1, arrived.shape[-1])
    return expert_forward(token_rows, inner_one, outer_one).reshape(arrived.shape)

def layer(operands):
    hidden, gain_row, inner_weight, outer_weight, chosen, weights = operands
    normed = normalize(hidden, gain_row).reshape(N_EXPERT, TOK_DEV, D)
    tables = jax.vmap(partial(slot_tables, experts=EXPERTS, capacity=CAP))
    token_at, filled, flat_slot, kept_choice = tables(chosen.reshape(N_EXPERT, TOK_DEV, TOP))
    taker = jax.vmap(partial(jnp.take, axis=0))
    outbound = taker(normed, token_at) * filled[:, :, :, None].astype(jnp.bfloat16)
    served = lax.map(serve_expert, (jnp.swapaxes(outbound, 0, 1), inner_weight, outer_weight))
    returned = jnp.swapaxes(served, 0, 1).reshape(N_EXPERT, EXPERTS * CAP, D)
    picked_rows = taker(returned, flat_slot)
    mixing = weights.reshape(N_EXPERT, TOK_DEV, TOP) * kept_choice.astype(weights.dtype)
    branch = jnp.einsum('btk,btkd->btd', mixing, picked_rows.astype(jnp.float32))
    return (hidden.astype(jnp.float32) + branch.reshape(TOKENS, D)).astype(jnp.bfloat16)

def reference(state, norm_gain, expert_in, expert_out, route_ids, route_weights):
    holding = state
    for tick_index in range(TICKS):
        moved = lax.map(layer, (holding, norm_gain, expert_in, expert_out, route_ids[tick_index], route_weights[tick_index]))
        holding = jnp.roll(moved, 1, axis=0)
    return holding
```

```python
import functools

import jax
import jax.numpy as jnp
from jax import lax
from jax.experimental import pallas as pl
from jax.experimental.pallas import tpu as pltpu
from jax.sharding import PartitionSpec as P

epsilon = 1e-06
CHUNKS = 4
MESH = pl.DeviceIdType.MESH


def relay_kernel(
    sections,
    experts,
    state_ref,
    gain_ref,
    win_hbm,
    wout_hbm,
    ids_ref,
    wts_ref,
    out_ref,
    win,
    wout,
    hcur,
    hrecv,
    gather,
    comb_send,
    comb_recv,
    sendbuf,
    recvbuf,
    acc,
    retsend,
    retrecv,
    win_sem,
    wout_sem,
    disp_ss,
    disp_rs,
    ret_ss,
    ret_rs,
    h_ss,
    h_rs,
    comb_ss,
    comb_rs,
):
    ticks = ids_ref.shape[0]
    top = ids_ref.shape[3]
    tokens = state_ref.shape[1]
    width = state_ref.shape[2]
    chunks = win.shape[0]
    cols = width // chunks
    hidden_units = wout.shape[0]
    capacity = tokens // 4
    slots = experts * capacity

    section = lax.axis_index("section")
    me = lax.axis_index("expert")
    after = lax.rem(section + 1, sections)
    before = lax.rem(section + sections - 1, sections)

    barrier = pltpu.get_barrier_semaphore()
    for d in range(1, experts):
        peer = lax.rem(me + d, experts)
        pl.semaphore_signal(
            barrier, inc=1, device_id={"section": section, "expert": peer}, device_id_type=MESH
        )
    for e in range(experts):
        for other in (after, before):
            pl.semaphore_signal(
                barrier, inc=1, device_id={"section": other, "expert": e}, device_id_type=MESH
            )

    def load_in(c):
        return pltpu.make_async_copy(
            win_hbm.at[0, 0, pl.ds(c * cols, cols)], win.at[c], win_sem.at[c]
        )

    load_out = pltpu.make_async_copy(wout_hbm.at[0, 0], wout, wout_sem)
    for c in range(chunks):
        load_in(c).start()
    load_out.start()

    lane = lax.broadcasted_iota(jnp.int32, (tokens, slots), 1)
    expert_of = jnp.zeros((tokens, slots), jnp.int32)
    for e in range(1, experts):
        expert_of = expert_of + (lane >= e * capacity).astype(jnp.int32)
    slot_of = (lane - expert_of * capacity).astype(jnp.float32)
    row_i = lax.broadcasted_iota(jnp.int32, (tokens, tokens), 0)
    col_i = lax.broadcasted_iota(jnp.int32, (tokens, tokens), 1)
    earlier = jnp.where(col_i < row_i, 1.0, 0.0).astype(jnp.bfloat16)

    def tables(t):
        ids = ids_ref[t, 0]
        wts = wts_ref[t, 0]
        hit = jnp.zeros((tokens, slots), jnp.float32)
        mix = jnp.zeros((tokens, slots), jnp.float32)
        for k in range(top):
            match = ids[:, k : k + 1] == expert_of
            hit = jnp.where(match, 1.0, hit)
            mix = jnp.where(match, wts[:, k : k + 1], mix)
        rank = jnp.dot(earlier, hit.astype(jnp.bfloat16), preferred_element_type=jnp.float32)
        keep = jnp.where(rank == slot_of, hit, 0.0)
        gather[t] = jnp.transpose(keep).astype(jnp.bfloat16)
        comb_send[t] = (keep * mix).astype(jnp.bfloat16)

    def comb_copy(t):
        return pltpu.make_async_remote_copy(
            src_ref=comb_send.at[t],
            dst_ref=comb_recv.at[t],
            send_sem=comb_ss.at[t],
            recv_sem=comb_rs.at[t],
            device_id={"section": after, "expert": me},
            device_id_type=MESH,
        )

    def h_copy(t, c):
        source = state_ref.at[0, :, pl.ds(c * cols, cols)] if t == 0 else hcur.at[t - 1, c]
        return pltpu.make_async_remote_copy(
            src_ref=source,
            dst_ref=hrecv.at[t, c],
            send_sem=h_ss.at[t, c],
            recv_sem=h_rs.at[t, c],
            device_id={"section": after, "expert": me},
            device_id_type=MESH,
        )

    def disp_copy(t, c, d):
        peer = lax.rem(me + d, experts)
        return pltpu.make_async_remote_copy(
            src_ref=sendbuf.at[t, c, pl.ds(peer * capacity, capacity)],
            dst_ref=recvbuf.at[t, c, pl.ds(me * capacity, capacity)],
            send_sem=disp_ss.at[t, c, d - 1],
            recv_sem=disp_rs.at[t, c, d - 1],
            device_id={"section": section, "expert": peer},
            device_id_type=MESH,
        )

    def disp_arrival(t, c, d):
        source = lax.rem(me + experts - d, experts)
        block = recvbuf.at[t, c, pl.ds(source * capacity, capacity)]
        return pltpu.make_async_remote_copy(
            src_ref=block,
            dst_ref=block,
            send_sem=disp_ss.at[t, c, d - 1],
            recv_sem=disp_rs.at[t, c, d - 1],
            device_id={"section": section, "expert": source},
            device_id_type=MESH,
        )

    def ret_copy(t, c, d):
        peer = lax.rem(me + d, experts)
        return pltpu.make_async_remote_copy(
            src_ref=retsend.at[t, c, pl.ds(peer * capacity, capacity)],
            dst_ref=retrecv.at[t, c, pl.ds(me * capacity, capacity)],
            send_sem=ret_ss.at[t, c, d],
            recv_sem=ret_rs.at[t, c, d],
            device_id={"section": after, "expert": peer},
            device_id_type=MESH,
        )

    def ret_arrival(t, c, d):
        source = lax.rem(me + experts - d, experts)
        block = retrecv.at[t, c, pl.ds(source * capacity, capacity)]
        return pltpu.make_async_remote_copy(
            src_ref=block,
            dst_ref=block,
            send_sem=ret_ss.at[t, c, d],
            recv_sem=ret_rs.at[t, c, d],
            device_id={"section": before, "expert": source},
            device_id_type=MESH,
        )

    def fill(t, c, chunk):
        rows = jnp.dot(gather[t], chunk, preferred_element_type=jnp.float32)
        sendbuf[t, c] = rows.astype(jnp.bfloat16)

    def keep_own(t, c):
        own = pl.ds(pl.multiple_of(me * capacity, capacity), capacity)
        recvbuf[t, c, own, :] = sendbuf[t, c, own, :]

    tables(0)
    fill(0, 0, state_ref[0, :, pl.ds(0, cols)])
    pl.semaphore_wait(barrier, experts - 1 + 2 * experts)
    for c in range(chunks):
        if c:
            fill(0, c, state_ref[0, :, pl.ds(c * cols, cols)])
        for d in range(1, experts):
            disp_copy(0, c, d).start()
        keep_own(0, c)
    comb_copy(0).start()
    for c in range(chunks):
        h_copy(0, c).start()
    for t in range(1, ticks):
        tables(t)
        comb_copy(t).start()

    for t in range(ticks):
        squares = jnp.zeros((slots, 1), jnp.float32)
        for c in range(chunks):
            if t == 0:
                load_in(c).wait()
            for d in range(1, experts):
                disp_arrival(t, c, d).wait_recv()
            wide = recvbuf[t, c].astype(jnp.float32)
            squares = squares + jnp.sum(wide * wide, axis=-1, keepdims=True)
            scaled = (wide * gain_ref[:, pl.ds(c * cols, cols)]).astype(jnp.bfloat16)
            part = jnp.dot(scaled, win[c], preferred_element_type=jnp.float32)
            if c == 0:
                acc[...] = part
            else:
                acc[...] += part
        rescale = lax.rsqrt(squares / width + epsilon)
        gate = acc[:, :hidden_units] * rescale
        up = acc[:, hidden_units:] * rescale
        activated = (gate / (1.0 + jnp.exp(-gate)) * up).astype(jnp.bfloat16)
        if t == 0:
            load_out.wait()
        for c in range(chunks):
            served = jnp.dot(
                activated, wout[:, pl.ds(c * cols, cols)], preferred_element_type=jnp.float32
            )
            retsend[t, c] = served.astype(jnp.bfloat16)
            for d in range(experts):
                ret_copy(t, c, d).start()
        for c in range(chunks):
            if c == 0:
                comb_copy(t).wait_recv()
            h_copy(t, c).wait_recv()
            for d in range(experts):
                ret_arrival(t, c, d).wait_recv()
            branch = jnp.dot(comb_recv[t], retrecv[t, c], preferred_element_type=jnp.float32)
            fresh = (hrecv[t, c].astype(jnp.float32) + branch).astype(jnp.bfloat16)
            if t == ticks - 1:
                out_ref[0, :, pl.ds(c * cols, cols)] = fresh
            else:
                hcur[t, c] = fresh
                fill(t + 1, c, fresh)
                for d in range(1, experts):
                    disp_copy(t + 1, c, d).start()
                h_copy(t + 1, c).start()
                keep_own(t + 1, c)

    for t in range(ticks):
        comb_copy(t).wait_send()
        for c in range(chunks):
            h_copy(t, c).wait_send()
            for d in range(experts):
                if d:
                    disp_copy(t, c, d).wait_send()
                ret_copy(t, c, d).wait_send()


def on_device(sections, experts, state, norm_gain, expert_in, expert_out, route_ids, route_weights):
    ticks = route_ids.shape[0]
    tokens, width = state.shape[1:]
    inner = expert_in.shape[3]
    hidden_units = expert_out.shape[2]
    slots = experts * (tokens // 4)
    cols = width // CHUNKS
    bf16 = jnp.bfloat16
    vmem = pl.BlockSpec(memory_space=pltpu.VMEM)
    hbm = pl.BlockSpec(memory_space=pl.ANY)
    dma = pltpu.SemaphoreType.DMA
    return pl.pallas_call(
        functools.partial(relay_kernel, sections, experts),
        out_shape=jax.ShapeDtypeStruct(state.shape, state.dtype),
        in_specs=[vmem, vmem, hbm, hbm, vmem, vmem],
        out_specs=vmem,
        scratch_shapes=[
            pltpu.VMEM((CHUNKS, cols, inner), bf16),
            pltpu.VMEM((hidden_units, width), bf16),
            pltpu.VMEM((max(ticks - 1, 1), CHUNKS, tokens, cols), bf16),
            pltpu.VMEM((ticks, CHUNKS, tokens, cols), bf16),
            pltpu.VMEM((ticks, slots, tokens), bf16),
            pltpu.VMEM((ticks, tokens, slots), bf16),
            pltpu.VMEM((ticks, tokens, slots), bf16),
            pltpu.VMEM((ticks, CHUNKS, slots, cols), bf16),
            pltpu.VMEM((ticks, CHUNKS, slots, cols), bf16),
            pltpu.VMEM((slots, inner), jnp.float32),
            pltpu.VMEM((ticks, CHUNKS, slots, cols), bf16),
            pltpu.VMEM((ticks, CHUNKS, slots, cols), bf16),
            dma((CHUNKS,)),
            dma,
            dma((ticks, CHUNKS, experts - 1)),
            dma((ticks, CHUNKS, experts - 1)),
            dma((ticks, CHUNKS, experts)),
            dma((ticks, CHUNKS, experts)),
            dma((ticks, CHUNKS)),
            dma((ticks, CHUNKS)),
            dma((ticks,)),
            dma((ticks,)),
        ],
        compiler_params=pltpu.CompilerParams(
            collective_id=0, has_side_effects=True, vmem_limit_bytes=60 * 1024 * 1024
        ),
        name="relay",
    )(state, norm_gain, expert_in, expert_out, route_ids, route_weights)


def solution(mesh):
    in_specs = (
        P("section", "expert", None),
        P("section", None),
        P("section", "expert", None, None),
        P("section", "expert", None, None),
        P(None, "section", "expert", None),
        P(None, "section", "expert", None),
    )
    out_specs = P("section", "expert", None)
    return jax.shard_map(
        functools.partial(on_device, mesh.shape["section"], mesh.shape["expert"]),
        mesh=mesh,
        in_specs=in_specs,
        out_specs=out_specs,
        check_vma=False,
    )
```

```python
import functools

import jax
import jax.numpy as jnp
from jax import lax
from jax.experimental import pallas as pl
from jax.experimental.pallas import tpu as pltpu
from jax.sharding import PartitionSpec as P

epsilon = 1e-06
CHUNKS = 4
PARTS = 2
LAG = 4
MESH = pl.DeviceIdType.MESH


def distances(experts):
    return list(range(1, experts))


def relay_kernel(
    sections,
    experts,
    state_ref,
    gain_ref,
    win_hbm,
    wout_hbm,
    ids_ref,
    wts_ref,
    out_ref,
    win,
    wout,
    hcur,
    hrecv,
    gather,
    comb_send,
    comb_recv,
    sendbuf,
    recvbuf,
    acc,
    retsend,
    retrecv,
    win_sem,
    wout_sem,
    disp_ss,
    disp_rs,
    ret_ss,
    ret_rs,
    h_ss,
    h_rs,
    comb_ss,
    comb_rs,
):
    ticks = ids_ref.shape[0]
    top = ids_ref.shape[1]
    tokens = state_ref.shape[1]
    width = state_ref.shape[2]
    chunks = win.shape[0]
    cols = width // chunks
    hidden_units = wout.shape[0]
    capacity = tokens // 4
    slots = experts * capacity
    parts = PARTS
    half = capacity // parts
    group = experts * half

    section = lax.axis_index("section")
    me = lax.axis_index("expert")
    after = lax.rem(section + 1, sections)
    before = lax.rem(section + sections - 1, sections)

    barrier = pltpu.get_barrier_semaphore()
    for d in range(1, experts):
        peer = lax.rem(me + d, experts)
        pl.semaphore_signal(
            barrier, inc=1, device_id={"section": section, "expert": peer}, device_id_type=MESH
        )
    for e in range(experts):
        for other in (after, before):
            pl.semaphore_signal(
                barrier, inc=1, device_id={"section": other, "expert": e}, device_id_type=MESH
            )

    def load_in(c):
        return pltpu.make_async_copy(
            win_hbm.at[0, 0, pl.ds(c * cols, cols)], win.at[c], win_sem.at[c]
        )

    load_out = pltpu.make_async_copy(wout_hbm.at[0, 0], wout, wout_sem)
    for c in range(chunks):
        load_in(c).start()
    load_out.start()

    slot_row = lax.broadcasted_iota(jnp.int32, (slots, tokens), 0)
    expert_of = jnp.zeros((slots, tokens), jnp.int32)
    slot_of = slot_row
    for p in range(parts):
        for e in range(experts):
            start = p * group + e * half
            inside = slot_row >= start
            expert_of = jnp.where(inside, e, expert_of)
            slot_of = jnp.where(inside, slot_row - start + p * half, slot_of)
    slot_of = slot_of.astype(jnp.float32)
    row_i = lax.broadcasted_iota(jnp.int32, (tokens, tokens), 0)
    col_i = lax.broadcasted_iota(jnp.int32, (tokens, tokens), 1)
    earlier = jnp.where(row_i < col_i, 1.0, 0.0).astype(jnp.bfloat16)

    def tables(t):
        hit = jnp.zeros((slots, tokens), jnp.float32)
        mix = jnp.zeros((slots, tokens), jnp.float32)
        for k in range(top):
            match = ids_ref[t, k] == expert_of
            hit = jnp.where(match, 1.0, hit)
            mix = jnp.where(match, wts_ref[t, k], mix)
        rank = jnp.dot(hit.astype(jnp.bfloat16), earlier, preferred_element_type=jnp.float32)
        keep = jnp.where(rank == slot_of, hit, 0.0)
        gather[t] = keep.astype(jnp.bfloat16)
        return keep * mix

    def comb_copy(t):
        return pltpu.make_async_remote_copy(
            src_ref=comb_send.at[t],
            dst_ref=comb_recv.at[t],
            send_sem=comb_ss.at[t],
            recv_sem=comb_rs.at[t],
            device_id={"section": after, "expert": me},
            device_id_type=MESH,
        )

    def send_comb(t, weighted):
        comb_send[t] = jnp.transpose(weighted).astype(jnp.bfloat16)
        comb_copy(t).start()

    def h_copy(t, c):
        source = state_ref.at[0, :, pl.ds(c * cols, cols)] if t == 0 else hcur.at[t - 1, c]
        return pltpu.make_async_remote_copy(
            src_ref=source,
            dst_ref=hrecv.at[t, c],
            send_sem=h_ss.at[t, c],
            recv_sem=h_rs.at[t, c],
            device_id={"section": after, "expert": me},
            device_id_type=MESH,
        )

    def send_rows(t, p, c):
        for d in distances(experts):
            peer = lax.rem(me + d, experts)
            pltpu.make_async_remote_copy(
                src_ref=sendbuf.at[t, c, pl.ds(p * group + peer * half, half)],
                dst_ref=recvbuf.at[t, c, pl.ds(p * group + me * half, half)],
                send_sem=disp_ss.at[t],
                recv_sem=disp_rs.at[t, p, c],
                device_id={"section": section, "expert": peer},
                device_id_type=MESH,
            ).start()

    def await_rows(t, p, c):
        block = recvbuf.at[t, c, pl.ds(p * group, group - half)]
        pltpu.make_async_remote_copy(
            src_ref=block,
            dst_ref=block,
            send_sem=disp_ss.at[t],
            recv_sem=disp_rs.at[t, p, c],
            device_id={"section": section, "expert": lax.rem(me + 1, experts)},
            device_id_type=MESH,
        ).wait_recv()

    def send_served(t, p, c):
        for d in distances(experts) + [0]:
            peer = lax.rem(me + d, experts)
            pltpu.make_async_remote_copy(
                src_ref=retsend.at[t, c, pl.ds(p * group + peer * half, half)],
                dst_ref=retrecv.at[t, c, pl.ds(p * group + me * half, half)],
                send_sem=ret_ss.at[t],
                recv_sem=ret_rs.at[t, c],
                device_id={"section": after, "expert": peer},
                device_id_type=MESH,
            ).start()

    def await_served(t, c):
        pltpu.make_async_remote_copy(
            src_ref=retrecv.at[t, c],
            dst_ref=retrecv.at[t, c],
            send_sem=ret_ss.at[t],
            recv_sem=ret_rs.at[t, c],
            device_id={"section": before, "expert": me},
            device_id_type=MESH,
        ).wait_recv()

    def fill(t, c, chunk):
        rows = jnp.dot(gather[t], chunk, preferred_element_type=jnp.float32)
        sendbuf[t, c] = rows.astype(jnp.bfloat16)

    def keep_own(t, c):
        for p in range(parts):
            own = pl.ds(pl.multiple_of(p * group + me * half, half), half)
            recvbuf[t, c, own, :] = sendbuf[t, c, own, :]

    def dispatch(t, c):
        send_rows(t, 0, c)
        for p in range(1, parts):
            late = c - p * LAG
            if late >= 0:
                send_rows(t, p, late)
        if c == chunks - 1:
            for p in range(1, parts):
                for late in range(max(chunks - p * LAG, 0), chunks):
                    send_rows(t, p, late)

    weighted = tables(0)
    for c in range(chunks):
        fill(0, c, state_ref[0, :, pl.ds(c * cols, cols)])
        if c == 0:
            pl.semaphore_wait(barrier, experts - 1 + 2 * experts)
        dispatch(0, c)
    for c in range(chunks):
        keep_own(0, c)
        h_copy(0, c).start()
    send_comb(0, weighted)
    for t in range(1, ticks):
        send_comb(t, tables(t))

    for t in range(ticks):
        for p in range(parts):
            rows = pl.ds(p * group, group)
            squares = jnp.zeros((group, 1), jnp.float32)
            for c in range(chunks):
                if t == 0 and p == 0:
                    load_in(c).wait()
                await_rows(t, p, c)
                wide = recvbuf[t, c, rows, :].astype(jnp.float32)
                squares = squares + jnp.sum(wide * wide, axis=-1, keepdims=True)
                scaled = (wide * gain_ref[:, pl.ds(c * cols, cols)]).astype(jnp.bfloat16)
                part = jnp.dot(scaled, win[c], preferred_element_type=jnp.float32)
                if c == 0:
                    acc[...] = part
                else:
                    acc[...] += part
            rescale = lax.rsqrt(squares / width + epsilon)
            gate = acc[:, :hidden_units] * rescale
            up = acc[:, hidden_units:] * rescale
            activated = (gate / (1.0 + jnp.exp(-gate)) * up).astype(jnp.bfloat16)
            if t == 0 and p == 0:
                load_out.wait()
            for c in range(chunks):
                served = jnp.dot(
                    activated, wout[:, pl.ds(c * cols, cols)], preferred_element_type=jnp.float32
                )
                retsend[t, c, rows, :] = served.astype(jnp.bfloat16)
                send_served(t, p, c)
        for c in range(chunks):
            if c == 0:
                comb_copy(t).wait_recv()
            h_copy(t, c).wait_recv()
            await_served(t, c)
            branch = jnp.dot(comb_recv[t], retrecv[t, c], preferred_element_type=jnp.float32)
            fresh = (hrecv[t, c].astype(jnp.float32) + branch).astype(jnp.bfloat16)
            if t == ticks - 1:
                out_ref[0, :, pl.ds(c * cols, cols)] = fresh
            else:
                hcur[t, c] = fresh
                fill(t + 1, c, fresh)
                dispatch(t + 1, c)
                h_copy(t + 1, c).start()
                keep_own(t + 1, c)

    for t in range(ticks):
        comb_copy(t).wait_send()
        for c in range(chunks):
            h_copy(t, c).wait_send()
        sent = sendbuf.at[t, :, pl.ds(0, slots - capacity)]
        pltpu.make_async_remote_copy(
            src_ref=sent,
            dst_ref=sent,
            send_sem=disp_ss.at[t],
            recv_sem=disp_rs.at[t, 0, 0],
            device_id={"section": after, "expert": me},
            device_id_type=MESH,
        ).wait_send()
        pltpu.make_async_remote_copy(
            src_ref=retsend.at[t],
            dst_ref=retrecv.at[t],
            send_sem=ret_ss.at[t],
            recv_sem=ret_rs.at[t, 0],
            device_id={"section": after, "expert": me},
            device_id_type=MESH,
        ).wait_send()


def on_device(sections, experts, state, norm_gain, expert_in, expert_out, route_ids, route_weights):
    ticks = route_ids.shape[0]
    tokens, width = state.shape[1:]
    inner = expert_in.shape[3]
    hidden_units = expert_out.shape[2]
    slots = experts * (tokens // 4)
    group = slots // PARTS
    cols = width // CHUNKS
    bf16 = jnp.bfloat16
    vmem = pl.BlockSpec(memory_space=pltpu.VMEM)
    hbm = pl.BlockSpec(memory_space=pl.ANY)
    dma = pltpu.SemaphoreType.DMA
    return pl.pallas_call(
        functools.partial(relay_kernel, sections, experts),
        out_shape=jax.ShapeDtypeStruct(state.shape, state.dtype),
        in_specs=[vmem, vmem, hbm, hbm, vmem, vmem],
        out_specs=vmem,
        scratch_shapes=[
            pltpu.VMEM((CHUNKS, cols, inner), bf16),
            pltpu.VMEM((hidden_units, width), bf16),
            pltpu.VMEM((max(ticks - 1, 1), CHUNKS, tokens, cols), bf16),
            pltpu.VMEM((ticks, CHUNKS, tokens, cols), bf16),
            pltpu.VMEM((ticks, slots, tokens), bf16),
            pltpu.VMEM((ticks, tokens, slots), bf16),
            pltpu.VMEM((ticks, tokens, slots), bf16),
            pltpu.VMEM((ticks, CHUNKS, slots, cols), bf16),
            pltpu.VMEM((ticks, CHUNKS, slots, cols), bf16),
            pltpu.VMEM((group, inner), jnp.float32),
            pltpu.VMEM((ticks, CHUNKS, slots, cols), bf16),
            pltpu.VMEM((ticks, CHUNKS, slots, cols), bf16),
            dma((CHUNKS,)),
            dma,
            dma((ticks,)),
            dma((ticks, PARTS, CHUNKS)),
            dma((ticks,)),
            dma((ticks, CHUNKS)),
            dma((ticks, CHUNKS)),
            dma((ticks, CHUNKS)),
            dma((ticks,)),
            dma((ticks,)),
        ],
        compiler_params=pltpu.CompilerParams(
            collective_id=0, has_side_effects=True, vmem_limit_bytes=60 * 1024 * 1024
        ),
        name="relay",
    )(
        state,
        norm_gain,
        expert_in,
        expert_out,
        jnp.transpose(route_ids, (0, 3, 1, 2)),
        jnp.transpose(route_weights, (0, 3, 1, 2)),
    )


def solution(mesh):
    in_specs = (
        P("section", "expert", None),
        P("section", None),
        P("section", "expert", None, None),
        P("section", "expert", None, None),
        P(None, "section", "expert", None),
        P(None, "section", "expert", None),
    )
    out_specs = P("section", "expert", None)
    return jax.shard_map(
        functools.partial(on_device, mesh.shape["section"], mesh.shape["expert"]),
        mesh=mesh,
        in_specs=in_specs,
        out_specs=out_specs,
        check_vma=False,
    )
```
